1024 devices in a mesh: gx: 32 (over x_hi, z, core), gy: 4 (over x_lo), gz: 8 (over y).
Axes of the slice: x: 8 (x_hi: 2, x_lo: 4; x = x_hi * 4 + x_lo), y: 8, z: 8, core: 2. Of those that a mesh axis runs over, the one named last changes fastest.
Arguments:
- density: float32 [128, 128, 1024], P('gx', 'gy', 'gz'), may hold values from 0.5 to 2
- velocity: float32 [3, 128, 128, 1024], P(None, 'gx', 'gy', 'gz'), may hold values from -2.5 to 2.5
- pressure: float32 [128, 128, 1024], P('gx', 'gy', 'gz'), may hold values from 0.5 to 2
Outputs:
- section_state: float32 [5, 128, 128, 1024], P(None, 'gx', 'gy', 'gz')
The draws below stay inside these ranges and needn't reach their ends.
All inputs are finite; a program needn't handle non-finite values.
Results may differ from the reference program's by a relative error of at most 0.0003.
Values sent between devices are 32-bit elements; how exact they have to be, the bound alone decides.
A program may use at most 32 MiB of HBM per device.

```python
import math
import jax
import jax.numpy as jnp
from jax import lax

CX = 4
NX = 128
NY = 128
NZ = 1024


def draw_velocity(key, part):
    growth = 1.0 + 2.0 * jnp.arange(NX, dtype=jnp.float32) / NX
    growth = growth[None, :, None, None]
    sample = jnp.clip(jax.random.normal(key, (3, NX, NY, NZ), jnp.float32), -2.5, 2.5)
    return 0.3 * growth * sample


def shard_levels(stream_key, shape, split, least, high):
    loudness = 1.0
    for position, shards_of in split:
        steps = jax.random.uniform(jax.random.fold_in(jax.random.fold_in(stream_key, 6), position), (shards_of,), jnp.float32, least / len(split), high / len(split))
        loudness = loudness * jnp.repeat(jnp.exp(steps), shape[position] // shards_of).reshape((-1,) + (1,) * (len(shape) - 1 - position))
    return loudness


def setup_inputs(seed: int = 0) -> dict:
    keys = jax.random.split(jax.random.key(seed), 4)
    return {
        "density": jnp.clip(jnp.exp(math.log(2.0) - 1.3862944 * jax.random.uniform(keys[0], (NX, NY, NZ), jnp.float32) ** shard_levels(keys[0], (NX, NY, NZ), ((0, 32), (1, 4), (2, 8)), -0.2, 0.2)), 0.5, 2.0),
        "velocity": draw_velocity(jax.random.fold_in(keys[3], 71), 0),
        "pressure": jnp.clip(jnp.exp(math.log(2.0) - 1.3862944 * jax.random.uniform(keys[2], (NX, NY, NZ), jnp.float32) ** shard_levels(keys[2], (NX, NY, NZ), ((0, 32), (1, 4), (2, 8)), -0.2, 0.2)), 0.5, 2.0),
    }


gamma_gas = 1.4
weno_eps = 1e-06
cfl_number = 0.4

def conserved(density, velocity, pressure):
    momenta = density[None] * velocity
    kinetic = 0.5 * density * lax.optimization_barrier(jnp.sum(velocity * velocity, axis=0))
    energy = pressure / (gamma_gas - 1.0) + kinetic
    return jnp.concatenate([density[None], momenta, energy[None]], axis=0)

def wave_speed(density, velocity, pressure):
    sound = jnp.sqrt(gamma_gas * pressure / density)
    return jnp.max(lax.optimization_barrier(jnp.sum(jnp.abs(velocity), axis=0)) + 3.0 * sound)

def combine(coeffs, arrays):
    total = None
    for coeff, array in zip(coeffs, arrays):
        if isinstance(coeff, float) and coeff == 0.0:
            continue
        term = coeff * array
        total = term if total is None else total + term
    return total

def weno_face(values):
    first, second, third, fourth, fifth = values
    cand_left = (2.0 * first - 7.0 * second + 11.0 * third) / 6.0
    cand_middle = (-second + 5.0 * third + 2.0 * fourth) / 6.0
    cand_right = (2.0 * third + 5.0 * fourth - fifth) / 6.0
    smooth_left = 13.0 / 12.0 * (first - 2.0 * second + third) ** 2 + 0.25 * (first - 4.0 * second + 3.0 * third) ** 2
    smooth_middle = 13.0 / 12.0 * (second - 2.0 * third + fourth) ** 2 + 0.25 * (second - fourth) ** 2
    smooth_right = 13.0 / 12.0 * (third - 2.0 * fourth + fifth) ** 2 + 0.25 * (3.0 * third - 4.0 * fourth + fifth) ** 2
    weight_left = 0.1 / (weno_eps + smooth_left) ** 2
    weight_middle = 0.6 / (weno_eps + smooth_middle) ** 2
    weight_right = 0.3 / (weno_eps + smooth_right) ** 2
    return (weight_left * cand_left + weight_middle * cand_middle + weight_right * cand_right) / (weight_left + weight_middle + weight_right)

def direction_flux(padded, field_dim, normal_comp):
    cells = padded.shape[field_dim + 1] - 6
    faces = cells + 1
    density = padded[0]
    energy = padded[4]
    velocity = [padded[1 + member] / density for member in range(3)]
    speed_sq = velocity[0] * velocity[0] + velocity[1] * velocity[1] + velocity[2] * velocity[2]
    pressure = (gamma_gas - 1.0) * (energy - 0.5 * density * speed_sq)
    sound_sq = gamma_gas * pressure / density
    sound = jnp.sqrt(sound_sq)
    enthalpy = (energy + pressure) / density
    normal_vel = velocity[normal_comp]
    others = [member for member in range(3) if member != normal_comp]
    order = [0, 1 + normal_comp, 1 + others[0], 1 + others[1], 4]
    state_perm = [padded[member] for member in order]
    flux_perm = [density * normal_vel, padded[1 + normal_comp] * normal_vel + pressure, padded[1 + others[0]] * normal_vel, padded[1 + others[1]] * normal_vel, (energy + pressure) * normal_vel]
    signal = jnp.abs(normal_vel) + sound

    def window(array, offset):
        return lax.slice_in_dim(array, offset, offset + faces, axis=field_dim)
    root_left = jnp.sqrt(window(density, 2))
    root_right = jnp.sqrt(window(density, 3))
    share_left = root_left / (root_left + root_right)
    share_right = root_right / (root_left + root_right)
    roe_vel = [share_left * window(member, 2) + share_right * window(member, 3) for member in velocity]
    roe_enth = share_left * window(enthalpy, 2) + share_right * window(enthalpy, 3)
    jump_sq = sum(((window(member, 3) - window(member, 2)) ** 2 for member in velocity))
    roe_sound_sq = share_left * window(sound_sq, 2) + share_right * window(sound_sq, 3) + 0.5 * (gamma_gas - 1.0) * share_left * share_right * jump_sq
    roe_sound = jnp.sqrt(roe_sound_sq)
    normal_roe = roe_vel[normal_comp]
    tang_first = roe_vel[others[0]]
    tang_second = roe_vel[others[1]]
    roe_qsq = normal_roe * normal_roe + tang_first * tang_first + tang_second * tang_second
    b_one = (gamma_gas - 1.0) / roe_sound_sq
    b_two = 0.5 * b_one * roe_qsq
    inv_sound = 1.0 / roe_sound
    left_rows = [[0.5 * (b_two + normal_roe * inv_sound), -0.5 * (b_one * normal_roe + inv_sound), -0.5 * b_one * tang_first, -0.5 * b_one * tang_second, 0.5 * b_one], [1.0 - b_two, b_one * normal_roe, b_one * tang_first, b_one * tang_second, -b_one], [-tang_first, 0.0, 1.0, 0.0, 0.0], [-tang_second, 0.0, 0.0, 1.0, 0.0], [0.5 * (b_two - normal_roe * inv_sound), -0.5 * (b_one * normal_roe - inv_sound), -0.5 * b_one * tang_first, -0.5 * b_one * tang_second, 0.5 * b_one]]
    right_rows = [[1.0, 1.0, 0.0, 0.0, 1.0], [normal_roe - roe_sound, normal_roe, 0.0, 0.0, normal_roe + roe_sound], [tang_first, tang_first, 1.0, 0.0, tang_first], [tang_second, tang_second, 0.0, 1.0, tang_second], [roe_enth - normal_roe * roe_sound, 0.5 * roe_qsq, tang_first, tang_second, roe_enth + normal_roe * roe_sound]]
    alpha = window(signal, 0)
    for offset in range(1, 6):
        alpha = jnp.maximum(alpha, window(signal, offset))
    plus_vals = [[None] * 6 for member in range(5)]
    minus_vals = [[None] * 6 for member in range(5)]
    for offset in range(6):
        state_here = [window(member, offset) for member in state_perm]
        flux_here = [window(member, offset) for member in flux_perm]
        for charac in range(5):
            char_state = combine(left_rows[charac], state_here)
            char_flux = combine(left_rows[charac], flux_here)
            plus_vals[charac][offset] = 0.5 * (char_flux + alpha * char_state)
            minus_vals[charac][offset] = 0.5 * (char_flux - alpha * char_state)
    hats = []
    for charac in range(5):
        upwind = weno_face(plus_vals[charac][0:5])
        downwind = weno_face([minus_vals[charac][5], minus_vals[charac][4], minus_vals[charac][3], minus_vals[charac][2], minus_vals[charac][1]])
        hats.append(upwind + downwind)
    face_flux = [None] * 5
    for member in range(5):
        face_flux[order[member]] = combine(right_rows[member], hats)
    result = [lax.slice_in_dim(member, 1, faces, axis=field_dim) - lax.slice_in_dim(member, 0, faces - 1, axis=field_dim) for member in face_flux]
    return jnp.stack(result, axis=0)

def reference(density, velocity, pressure):
    state = conserved(density, velocity, pressure)
    step = cfl_number / wave_speed(density, velocity, pressure)
    padded = jnp.pad(state, ((0, 0), (3, 3), (3, 3), (3, 3)), mode='wrap')

    def slab_update(start):
        piece = lax.dynamic_slice_in_dim(padded, start, CX + 6, axis=1)
        total = direction_flux(piece[:, :, 3:-3, 3:-3], 0, 0)
        total = total + direction_flux(piece[:, 3:-3, :, 3:-3], 1, 1)
        total = total + direction_flux(piece[:, 3:-3, 3:-3, :], 2, 2)
        return total
    starts = jnp.arange(NX // CX, dtype=jnp.int32) * CX
    slabs = lax.map(slab_update, starts)
    total = jnp.moveaxis(slabs, 0, 1).reshape(5, NX, NY, NZ)
    return state - step * total
```

```python
import jax
import jax.numpy as jnp
from jax import lax
from jax.experimental import pallas as pl
from jax.experimental.pallas import tpu as pltpu
from jax.sharding import PartitionSpec as P

gamma_gas = 1.4
weno_eps = 1e-06
cfl_number = 0.4

MESH = pl.DeviceIdType.MESH

U0, UN, UA, UB, UE, FN, FA, FB, FE, ROOT, VN, VA, VB, ENTH, SOUND, SIGNAL = range(16)
ORDER = ((0, 1, 2), (1, 0, 2), (2, 0, 1))


def cell_values(density, normal, first, second, pressure):
    inv = 1.0 / density
    sound_sq = gamma_gas * pressure * inv
    sound = jnp.sqrt(sound_sq)
    half_sq = 0.5 * (normal * normal + first * first + second * second)
    energy = pressure * (1.0 / (gamma_gas - 1.0)) + density * half_sq
    total = energy + pressure
    mom_n = density * normal
    values = [None] * 16
    values[U0] = density
    values[UN] = mom_n
    values[UA] = density * first
    values[UB] = density * second
    values[UE] = energy
    values[FN] = mom_n * normal + pressure
    values[FA] = mom_n * first
    values[FB] = mom_n * second
    values[FE] = total * normal
    values[ROOT] = jnp.sqrt(density)
    values[VN] = normal
    values[VA] = first
    values[VB] = second
    values[ENTH] = total * inv
    values[SOUND] = sound_sq
    values[SIGNAL] = jnp.abs(normal) + sound
    return values, sound


def weno_part(d0, d1, d2, d3, eps):
    s1 = d1 - d0
    s2 = d2 - d1
    s3 = d3 - d2
    f1 = 0.75 * d1
    f2 = 0.75 * d2
    b0 = s1 * s1 + f1 * (d1 + s1) + eps
    b1 = s2 * s2 + f1 * d2 + eps
    b2 = s3 * s3 + f2 * (d2 - s3) + eps
    g0 = b1 * b2
    g1 = b0 * b2
    g2 = b0 * b1
    w0 = g0 * g0
    w1 = g1 * g1
    w2 = 3.0 * (g2 * g2)
    total = w0 + 6.0 * w1 + w2
    top = 2.0 * (w0 * (s1 - s2)) + w2 * (s2 - s3)
    return top / total


def face_block(load):
    alpha = load(SIGNAL, 0)
    for k in range(1, 6):
        alpha = jnp.maximum(alpha, load(SIGNAL, k))
    root_l = load(ROOT, 2)
    root_r = load(ROOT, 3)
    inv_sum = 1.0 / (root_l + root_r)
    wl = root_l * inv_sum
    wr = root_r * inv_sum
    vel = []
    jump_sq = None
    for member in (VN, VA, VB):
        left, right = load(member, 2), load(member, 3)
        vel.append(wl * left + wr * right)
        jump = right - left
        jump_sq = jump * jump if jump_sq is None else jump_sq + jump * jump
    un, ta, tb = vel
    enth = wl * load(ENTH, 2) + wr * load(ENTH, 3)
    sound_sq = (
        wl * load(SOUND, 2)
        + wr * load(SOUND, 3)
        + (0.5 * (gamma_gas - 1.0)) * (wl * wr) * jump_sq
    )
    sound = jnp.sqrt(sound_sq)
    inv_sound = 1.0 / sound
    b_one = (gamma_gas - 1.0) * inv_sound * inv_sound
    half_sq = 0.5 * (un * un + ta * ta + tb * tb)

    plus = [[None] * 5 for _ in range(4)]
    minus = [[None] * 5 for _ in range(4)]
    linear = []
    for comp in range(5):
        state = [load(U0 + comp, k) for k in range(6)]
        flux = [load(UN if comp == 0 else FN + comp - 1, k) for k in range(6)]
        for k in range(5):
            df = flux[k + 1] - flux[k]
            du = alpha * (state[k + 1] - state[k])
            if k < 4:
                plus[k][comp] = df + du
            if k > 0:
                minus[k - 1][comp] = df - du
        linear.append(
            6.0 * (flux[2] + flux[3])
            + ((plus[1][comp] - minus[2][comp]) + (minus[1][comp] - plus[2][comp]))
        )

    def project(vector):
        r, n, a, b, e = vector
        n_rel = n - un * r
        a_rel = a - ta * r
        b_rel = b - tb * r
        inner = e - (un * n_rel + ta * a_rel + tb * b_rel + half_sq * r)
        press = b_one * inner
        wave = n_rel * inv_sound
        return press - wave, r - press, a_rel, b_rel, press + wave

    plus = [project(vector) for vector in plus]
    minus = [project(vector) for vector in minus]
    hats = []
    for charac in range(5):
        scale = 16.0 if charac in (0, 4) else 4.0
        eps = 0.75 * scale * weno_eps
        up = weno_part(*(plus[k][charac] for k in (0, 1, 2, 3)), eps)
        down = weno_part(*(minus[k][charac] for k in (3, 2, 1, 0)), eps)
        hats.append(up - down)
    both = 0.5 * (hats[0] + hats[4])
    split = (0.5 * sound) * (hats[4] - hats[0])
    dens = both + hats[1]
    return [
        linear[0] + dens,
        linear[1] + (un * dens + split),
        linear[2] + (ta * dens + hats[2]),
        linear[3] + (tb * dens + hats[3]),
        linear[4]
        + (enth * both + un * split + half_sq * hats[1] + ta * hats[2] + tb * hats[3]),
    ]


def peers():
    gx = lax.axis_index("gx")
    gy = lax.axis_index("gy")
    gz = lax.axis_index("gz")
    core = gx % 2
    z = (gx // 2) % 8
    x_hi = gx // 16

    def at(x_hi, gy, z, core, gz):
        return {"gx": x_hi * 16 + z * 2 + core, "gy": gy, "gz": gz}

    lines = [[], [], []]
    for step in range(8):
        for flip in range(2):
            if step or flip:
                lines[0].append(at(x_hi, gy, z, (core + flip) % 2, (gz + step) % 8))
    for step in range(1, 8):
        lines[1].append(at(x_hi, gy, (z + step) % 8, core, gz))
    for step in range(1, 8):
        x = (x_hi * 4 + gy + step) % 8
        lines[2].append(at(x // 4, x % 4, z, core, gz))
    halos = []
    for shift in (1, -1):
        halos.append(
            (
                {"gx": (gx + shift + 32) % 32, "gy": gy, "gz": gz},
                {"gx": gx, "gy": (gy + shift + 4) % 4, "gz": gz},
                {"gx": gx, "gy": gy, "gz": (gz + shift + 8) % 8},
            )
        )
    far = {"gx": (gx + 31 + 2 * core) % 32, "gy": gy, "gz": gz}
    return lines, halos, far


def kernel(
    dens_ref,
    vel_ref,
    pres_ref,
    out_ref,
    raw_x,
    raw_y,
    raw_z,
    cell_x,
    cell_y,
    cell_z,
    flux_x,
    flux_y,
    flux_z,
    total,
    tops,
    top_in,
    load_sem,
    max_send,
    max_recv,
    halo_send,
    halo_recv,
):
    lines, halos, far = peers()
    barrier = pltpu.get_barrier_semaphore()
    loads = [
        pltpu.make_async_copy(dens_ref, raw_x.at[0, pl.ds(96, 128)], load_sem.at[0]),
        pltpu.make_async_copy(vel_ref.at[0], raw_x.at[1, pl.ds(96, 128)], load_sem.at[1]),
        pltpu.make_async_copy(vel_ref.at[1], raw_x.at[2, pl.ds(96, 128)], load_sem.at[2]),
        pltpu.make_async_copy(vel_ref.at[2], raw_x.at[3, pl.ds(96, 128)], load_sem.at[3]),
        pltpu.make_async_copy(pres_ref, raw_x.at[4, pl.ds(96, 128)], load_sem.at[4]),
    ]
    for copy in loads:
        copy.start()
    greeted = lines[0] + lines[1] + lines[2] + [far]
    for device in greeted:
        pl.semaphore_signal(barrier, inc=1, device_id=device, device_id_type=MESH)
    for copy in loads:
        copy.wait()

    def cells(raw, cell, direction, start, blocks):
        first, second, third = ORDER[direction]

        def body(block, carry):
            rows = pl.ds(pl.multiple_of(start + 8 * block, 8), 8)
            values, sound = cell_values(
                raw[0, rows, :],
                raw[1 + first, rows, :],
                raw[1 + second, rows, :],
                raw[1 + third, rows, :],
                raw[4, rows, :],
            )
            for index, value in enumerate(values):
                cell[index, rows, :] = value
            speed = (
                jnp.abs(values[VN]) + jnp.abs(values[VA]) + jnp.abs(values[VB]) + 3.0 * sound
            )
            return jnp.maximum(carry, speed)

        return lax.fori_loop(0, blocks, body, jnp.zeros((8, 128), jnp.float32))

    def faces(cell, flux, stride, start, blocks):
        def body(block, carry):
            base = pl.multiple_of(start + 8 * block, 8)

            def load(index, k):
                return cell[index, pl.ds(base + (k - 2) * stride, 8), :]

            for comp, value in enumerate(face_block(load)):
                flux[comp, pl.ds(base, 8), :] = value
            return carry

        lax.fori_loop(0, blocks, body, 0)

    local = cells(raw_x, cell_x, 0, 96, 16)
    tops[0] = jnp.max(local, axis=0, keepdims=True)

    for field in range(5):
        for x in range(4):
            for part in range(4):
                raw_y[field, pl.ds(16 + 32 * part + x, 8, stride=4), :] = raw_x[
                    field, pl.ds(96 + 32 * x + 8 * part, 8), :
                ]
        raw_z[field, pl.ds(16, 128), :] = raw_x[field, pl.ds(96, 128), :].T

    pl.semaphore_wait(barrier, len(greeted))

    def send_tops(phase):
        first = (0, 15, 22)[phase]
        copies = []
        for slot, device in enumerate(lines[phase]):
            copies.append(
                pltpu.make_async_remote_copy(
                    src_ref=tops.at[phase],
                    dst_ref=top_in.at[first + slot],
                    send_sem=max_send.at[first + slot],
                    recv_sem=max_recv.at[first + slot],
                    device_id=device,
                    device_id_type=MESH,
                )
            )
        for copy in copies:
            copy.start()
        return copies

    def gather_tops(phase, copies):
        first = (0, 15, 22)[phase]
        for copy in copies:
            copy.wait()
        top = tops[phase]
        for slot in range(len(copies)):
            top = jnp.maximum(top, top_in[first + slot])
        return top

    top_copies = send_tops(0)

    def send_halos(direction):
        raw, tail, tail_to, head, head_to, size = (
            (raw_x, 128, 0, 96, 224, 96),
            (raw_y, 128, 0, 16, 144, 16),
            (raw_z, 136, 8, 16, 144, 8),
        )[direction]
        copies = []
        for side, (source, target) in enumerate(((tail, tail_to), (head, head_to))):
            copies.append(
                pltpu.make_async_remote_copy(
                    src_ref=raw.at[:, pl.ds(source, size)],
                    dst_ref=raw.at[:, pl.ds(target, size)],
                    send_sem=halo_send.at[2 * direction + side],
                    recv_sem=halo_recv.at[2 * direction + side],
                    device_id=halos[side][direction],
                    device_id_type=MESH,
                )
            )
        for copy in copies:
            copy.start()
        return copies

    halo_z = send_halos(2)
    halo_y = send_halos(1)
    halo_x = send_halos(0)

    cells(raw_z, cell_z, 2, 16, 16)
    cells(raw_y, cell_y, 1, 16, 16)

    for copy in halo_z:
        copy.wait()
    cells(raw_z, cell_z, 2, 8, 1)
    cells(raw_z, cell_z, 2, 144, 1)
    faces(cell_z, flux_z, 1, 8, 17)

    tops[1] = gather_tops(0, top_copies)
    top_copies = send_tops(1)

    for copy in halo_y:
        copy.wait()
    cells(raw_y, cell_y, 1, 0, 2)
    cells(raw_y, cell_y, 1, 144, 2)
    faces(cell_y, flux_y, 4, 8, 17)

    tops[2] = gather_tops(1, top_copies)
    top_copies = send_tops(2)

    for comp in range(5):
        along_z = flux_z[comp_at(2, comp), pl.ds(16, 128), :] - flux_z[
            comp_at(2, comp), pl.ds(15, 128), :
        ]
        total[comp] = along_z.T
        along_y = comp_at(1, comp)
        for part in range(16):
            rows = pl.ds(16 + 8 * part, 8)
            flux_x[0, rows, :] = (
                flux_y[along_y, rows, :] - flux_y[along_y, pl.ds(12 + 8 * part, 8), :]
            )
        for x in range(4):
            for part in range(4):
                rows = pl.ds(32 * x + 8 * part, 8)
                total[comp, rows, :] = (
                    total[comp, rows, :]
                    + flux_x[0, pl.ds(16 + 32 * part + x, 8, stride=4), :]
                )

    for copy in halo_x:
        copy.wait()
    cells(raw_x, cell_x, 0, 0, 12)
    cells(raw_x, cell_x, 0, 224, 12)
    faces(cell_x, flux_x, 32, 64, 20)

    top = gather_tops(2, top_copies)
    step = (cfl_number / 12.0) / jnp.max(top, axis=1, keepdims=True)
    for comp in range(5):
        for part in range(16):
            rows = pl.ds(8 * part, 8)
            change = total[comp, rows, :] + (
                flux_x[comp, pl.ds(96 + 8 * part, 8), :]
                - flux_x[comp, pl.ds(64 + 8 * part, 8), :]
            )
            out_ref[comp, rows, :] = cell_x[comp, pl.ds(96 + 8 * part, 8), :] - step * change


def comp_at(direction, comp):
    if comp in (0, 4):
        return comp
    return 1 + ORDER[direction].index(comp - 1)


def local(density, velocity, pressure):
    f32 = jnp.float32
    result = pl.pallas_call(
        kernel,
        name="section",
        out_shape=jax.ShapeDtypeStruct((5, 128, 128), f32),
        in_specs=[pl.BlockSpec(memory_space=pltpu.HBM)] * 3,
        out_specs=pl.BlockSpec(memory_space=pltpu.VMEM),
        scratch_shapes=[
            pltpu.VMEM((5, 320, 128), f32),
            pltpu.VMEM((5, 160, 128), f32),
            pltpu.VMEM((5, 160, 128), f32),
            pltpu.VMEM((16, 320, 128), f32),
            pltpu.VMEM((16, 160, 128), f32),
            pltpu.VMEM((16, 160, 128), f32),
            pltpu.VMEM((5, 224, 128), f32),
            pltpu.VMEM((5, 144, 128), f32),
            pltpu.VMEM((5, 144, 128), f32),
            pltpu.VMEM((5, 128, 128), f32),
            pltpu.VMEM((3, 1, 128), f32),
            pltpu.VMEM((29, 1, 128), f32),
            pltpu.SemaphoreType.DMA((5,)),
            pltpu.SemaphoreType.DMA((29,)),
            pltpu.SemaphoreType.DMA((29,)),
            pltpu.SemaphoreType.DMA((6,)),
            pltpu.SemaphoreType.DMA((6,)),
        ],
        compiler_params=pltpu.CompilerParams(collective_id=0, has_side_effects=True),
    )(
        density.reshape(128, 128),
        velocity.reshape(3, 128, 128),
        pressure.reshape(128, 128),
    )
    return result.reshape(5, 4, 32, 128)


def solution(mesh):
    return jax.shard_map(
        local,
        mesh=mesh,
        in_specs=(P("gx", "gy", "gz"), P(None, "gx", "gy", "gz"), P("gx", "gy", "gz")),
        out_specs=P(None, "gx", "gy", "gz"),
        check_vma=False,
    )
```

```python
import jax
import jax.numpy as jnp
from jax import lax
from jax.experimental import pallas as pl
from jax.experimental.pallas import tpu as pltpu
from jax.sharding import PartitionSpec as P

gamma_gas = 1.4
weno_eps = 1e-06
cfl_number = 0.4

MESH = pl.DeviceIdType.MESH

U0, UN, UA, UB, UE, FN, FA, FB, FE, ROOT, VN, VA, VB, ENTH, SOUND, SIGNAL = range(16)
ORDER = ((0, 1, 2), (1, 0, 2), (2, 0, 1))


def cell_values(density, normal, first, second, pressure):
    inv = 1.0 / density
    sound_sq = gamma_gas * pressure * inv
    sound = jnp.sqrt(sound_sq)
    half_sq = 0.5 * (normal * normal + first * first + second * second)
    energy = pressure * (1.0 / (gamma_gas - 1.0)) + density * half_sq
    total = energy + pressure
    mom_n = density * normal
    values = [None] * 16
    values[U0] = density
    values[UN] = mom_n
    values[UA] = density * first
    values[UB] = density * second
    values[UE] = energy
    values[FN] = mom_n * normal + pressure
    values[FA] = mom_n * first
    values[FB] = mom_n * second
    values[FE] = total * normal
    values[ROOT] = jnp.sqrt(density)
    values[VN] = normal
    values[VA] = first
    values[VB] = second
    values[ENTH] = total * inv
    values[SOUND] = sound_sq
    values[SIGNAL] = jnp.abs(normal) + sound
    return values


def weno_part(d0, d1, d2, d3, eps):
    s1 = d1 - d0
    s2 = d2 - d1
    s3 = d3 - d2
    f1 = 0.75 * d1
    f2 = 0.75 * d2
    b0 = s1 * s1 + f1 * (d1 + s1) + eps
    b1 = s2 * s2 + f1 * d2 + eps
    b2 = s3 * s3 + f2 * (d2 - s3) + eps
    g0 = b1 * b2
    g1 = b0 * b2
    g2 = b0 * b1
    w0 = g0 * g0
    w1 = g1 * g1
    w2 = 3.0 * (g2 * g2)
    total = w0 + 6.0 * w1 + w2
    top = 2.0 * (w0 * (s1 - s2)) + w2 * (s2 - s3)
    return top / total


def face_block(load):
    alpha = load(SIGNAL, 0)
    for k in range(1, 6):
        alpha = jnp.maximum(alpha, load(SIGNAL, k))
    root_l = load(ROOT, 2)
    root_r = load(ROOT, 3)
    inv_sum = 1.0 / (root_l + root_r)
    wl = root_l * inv_sum
    wr = root_r * inv_sum
    vel = []
    jump_sq = None
    for member in (VN, VA, VB):
        left, right = load(member, 2), load(member, 3)
        vel.append(wl * left + wr * right)
        jump = right - left
        jump_sq = jump * jump if jump_sq is None else jump_sq + jump * jump
    un, ta, tb = vel
    enth = wl * load(ENTH, 2) + wr * load(ENTH, 3)
    sound_sq = (
        wl * load(SOUND, 2)
        + wr * load(SOUND, 3)
        + (0.5 * (gamma_gas - 1.0)) * (wl * wr) * jump_sq
    )
    sound = jnp.sqrt(sound_sq)
    inv_sound = 1.0 / sound
    b_one = (gamma_gas - 1.0) * inv_sound * inv_sound
    half_sq = 0.5 * (un * un + ta * ta + tb * tb)

    plus = [[None] * 5 for _ in range(4)]
    minus = [[None] * 5 for _ in range(4)]
    linear = []
    for comp in range(5):
        state = [load(U0 + comp, k) for k in range(6)]
        flux = [load(UN if comp == 0 else FN + comp - 1, k) for k in range(6)]
        for k in range(5):
            df = flux[k + 1] - flux[k]
            du = alpha * (state[k + 1] - state[k])
            if k < 4:
                plus[k][comp] = df + du
            if k > 0:
                minus[k - 1][comp] = df - du
        linear.append(
            6.0 * (flux[2] + flux[3])
            + ((plus[1][comp] - minus[2][comp]) + (minus[1][comp] - plus[2][comp]))
        )

    def project(vector):
        r, n, a, b, e = vector
        n_rel = n - un * r
        a_rel = a - ta * r
        b_rel = b - tb * r
        inner = e - (un * n_rel + ta * a_rel + tb * b_rel + half_sq * r)
        press = b_one * inner
        wave = n_rel * inv_sound
        return press - wave, r - press, a_rel, b_rel, press + wave

    plus = [project(vector) for vector in plus]
    minus = [project(vector) for vector in minus]
    hats = []
    for charac in range(5):
        scale = 16.0 if charac in (0, 4) else 4.0
        eps = 0.75 * scale * weno_eps
        up = weno_part(*(plus[k][charac] for k in (0, 1, 2, 3)), eps)
        down = weno_part(*(minus[k][charac] for k in (3, 2, 1, 0)), eps)
        hats.append(up - down)
    both = 0.5 * (hats[0] + hats[4])
    split = (0.5 * sound) * (hats[4] - hats[0])
    dens = both + hats[1]
    return [
        linear[0] + dens,
        linear[1] + (un * dens + split),
        linear[2] + (ta * dens + hats[2]),
        linear[3] + (tb * dens + hats[3]),
        linear[4]
        + (enth * both + un * split + half_sq * hats[1] + ta * hats[2] + tb * hats[3]),
    ]


def place_of():
    gx = lax.axis_index("gx")
    return gx % 2, (gx // 2) % 8, (gx // 16) * 4 + lax.axis_index("gy"), lax.axis_index("gz")


def device(core, place, across, gz):
    return {"gx": (across // 4) * 16 + place * 2 + core, "gy": across % 4, "gz": gz}


def neighbours():
    gx, gy, gz = (lax.axis_index(name) for name in ("gx", "gy", "gz"))
    found = []
    for shift in (1, -1):
        found.append(
            (
                {"gx": (gx + shift + 32) % 32, "gy": gy, "gz": gz},
                {"gx": gx, "gy": (gy + shift + 4) % 4, "gz": gz},
                {"gx": gx, "gy": gy, "gz": (gz + shift + 8) % 8},
            )
        )
    return found


STEPS = [(i, j) for i in range(8) for j in range(8) if i or j]
STEPS.sort(key=lambda ij: -min(ij[0], 8 - ij[0]) - min(ij[1], 8 - ij[1]))
PLANE, FINAL = 16, 16 + 63


def kernel(
    dens_ref,
    vel_ref,
    pres_ref,
    out_ref,
    raw_x,
    raw_y,
    raw_z,
    cell_x,
    cell_y,
    cell_z,
    flux_x,
    flux_y,
    flux_z,
    total,
    tops,
    top_in,
    load_sem,
    max_send,
    max_recv,
    halo_send,
    halo_recv,
):
    core, place, across, gz = place_of()
    first_place = place == 0
    other_place = place != 0
    early = place < 4
    loads = [
        pltpu.make_async_copy(dens_ref, raw_x.at[0, pl.ds(96, 128)], load_sem.at[0]),
        pltpu.make_async_copy(pres_ref, raw_x.at[4, pl.ds(96, 128)], load_sem.at[4]),
        pltpu.make_async_copy(vel_ref.at[0], raw_x.at[1, pl.ds(96, 128)], load_sem.at[1]),
        pltpu.make_async_copy(vel_ref.at[1], raw_x.at[2, pl.ds(96, 128)], load_sem.at[2]),
        pltpu.make_async_copy(vel_ref.at[2], raw_x.at[3, pl.ds(96, 128)], load_sem.at[3]),
    ]
    for copy in loads:
        copy.start()

    barrier = pltpu.get_barrier_semaphore()

    def greet(to):
        pl.semaphore_signal(barrier, inc=1, device_id=to, device_id_type=MESH)

    @pl.when(other_place)
    def _():
        for side in neighbours():
            for to in side:
                greet(to)
        greet(device(core, 0, across, gz))

    @pl.when(first_place)
    def _():
        for side in neighbours():
            for to in side:
                greet(to)
        for step in range(1, 8):
            for flip in range(2):
                greet(device((core + flip) % 2, step, across, gz))
        for i, j in STEPS:
            greet(device(core, place, (across + i) % 8, (gz + j) % 8))

    for copy in loads:
        copy.wait()

    local = None
    for part in range(16):
        rows = pl.ds(96 + 8 * part, 8)
        sound = jnp.sqrt(gamma_gas * raw_x[4, rows, :] / raw_x[0, rows, :])
        speed = (
            jnp.abs(raw_x[1, rows, :]) + jnp.abs(raw_x[2, rows, :]) + jnp.abs(raw_x[3, rows, :])
        ) + 3.0 * sound
        local = speed if local is None else jnp.maximum(local, speed)
    tops[0] = jnp.max(local, axis=0, keepdims=True)

    def cells(raw, cell, direction, start, blocks):
        first, second, third = ORDER[direction]

        def body(block, carry):
            rows = pl.ds(pl.multiple_of(start + 8 * block, 8), 8)
            values = cell_values(
                raw[0, rows, :],
                raw[1 + first, rows, :],
                raw[1 + second, rows, :],
                raw[1 + third, rows, :],
                raw[4, rows, :],
            )
            for index, value in enumerate(values):
                cell[index, rows, :] = value
            return carry

        lax.fori_loop(0, blocks, body, 0)

    def faces(cell, flux, stride, start, blocks):
        def body(block, carry):
            base = pl.multiple_of(start + 8 * block, 8)

            def load(index, k):
                return cell[index, pl.ds(base + (k - 2) * stride, 8), :]

            for comp, value in enumerate(face_block(load)):
                flux[comp, pl.ds(base, 8), :] = value
            return carry

        lax.fori_loop(0, blocks, body, 0)

    def relayout():
        for field in range(5):
            for x in range(4):
                for part in range(4):
                    raw_y[field, pl.ds(16 + 32 * part + x, 8, stride=4), :] = raw_x[
                        field, pl.ds(96 + 32 * x + 8 * part, 8), :
                    ]
            raw_z[field, pl.ds(16, 128), :] = raw_x[field, pl.ds(96, 128), :].T
        cells(raw_x, cell_x, 0, 96, 16)

    def interior():
        cells(raw_z, cell_z, 2, 16, 16)
        cells(raw_y, cell_y, 1, 16, 16)
        faces(cell_z, flux_z, 1, 24, 14)
        faces(cell_y, flux_y, 4, 24, 13)

    def top_copy(source, slot, sent, to):
        return pltpu.make_async_remote_copy(
            src_ref=tops.at[source],
            dst_ref=top_in.at[slot],
            send_sem=max_send.at[sent],
            recv_sem=max_recv.at[slot],
            device_id=to,
            device_id_type=MESH,
        )

    def first_copy(flip):
        return top_copy(
            0, 2 * place + flip, flip, device((core + flip) % 2, 0, across, gz)
        )

    def plane_copies():
        return [
            top_copy(
                1, PLANE + k, PLANE + k, device(core, place, (across + i) % 8, (gz + j) % 8)
            )
            for k, (i, j) in enumerate(STEPS)
        ]

    def final_copies():
        return [
            top_copy(2, FINAL, 1 + step, device(core, step, across, gz)) for step in range(1, 8)
        ]

    def halo_copy(raw, source, target, size, slot, to):
        return pltpu.make_async_remote_copy(
            src_ref=raw.at[:, pl.ds(source, size)],
            dst_ref=raw.at[:, pl.ds(target, size)],
            send_sem=halo_send.at[slot],
            recv_sem=halo_recv.at[slot],
            device_id=to,
            device_id_type=MESH,
        )

    (next_x, next_y, next_z), (last_x, last_y, last_z) = neighbours()
    halo_z = [
        halo_copy(raw_z, 136, 8, 8, 0, next_z),
        halo_copy(raw_z, 16, 144, 8, 1, last_z),
    ]
    halo_y = [
        halo_copy(raw_y, 128, 0, 16, 2, next_y),
        halo_copy(raw_y, 16, 144, 16, 3, last_y),
    ]
    head_x = halo_copy(raw_x, 96, 224, 96, 4, last_x)
    tail_x = [
        halo_copy(raw_x, 128 + 32 * plane, 32 * plane, 32, 5 + plane, next_x)
        for plane in (2, 1, 0)
    ]

    @pl.when(early)
    def _():
        relayout()
        interior()

    pl.semaphore_wait(barrier, jnp.where(first_place, 6 + 7 + len(STEPS), 6 + 2))

    @pl.when(other_place)
    def _():
        for flip in range(2):
            first_copy(flip).start()

    @pl.when(first_place)
    def _():
        first_copy(1).start()

    for copy in tail_x:
        copy.start()
    held = jnp.logical_and(first_place, core == 0)

    @pl.when(jnp.logical_not(held))
    def _():
        head_x.start()

    @pl.when(jnp.logical_not(early))
    def _():
        relayout()

    for copy in halo_z:
        copy.start()

    @pl.when(early)
    def _():
        for copy in halo_y:
            copy.start()

    @pl.when(jnp.logical_not(early))
    def _():
        interior()
        for copy in halo_y:
            copy.start()

    @pl.when(first_place)
    def _():
        for slot in range(1, 16):
            top_copy(0, slot, 0, device(core, place, across, gz)).wait_recv()
        top = tops[0]
        for slot in range(1, 16):
            top = jnp.maximum(top, top_in[slot])
        tops[1] = top
        for copy in plane_copies():
            copy.start()

    @pl.when(held)
    def _():
        head_x.start()

    for copy in halo_z:
        copy.wait_recv()
    cells(raw_z, cell_z, 2, 8, 1)
    cells(raw_z, cell_z, 2, 144, 1)
    faces(cell_z, flux_z, 1, 8, 2)
    faces(cell_z, flux_z, 1, 136, 1)
    for copy in halo_y:
        copy.wait_recv()
    cells(raw_y, cell_y, 1, 0, 2)
    cells(raw_y, cell_y, 1, 144, 2)
    faces(cell_y, flux_y, 4, 8, 2)
    faces(cell_y, flux_y, 4, 128, 2)

    for comp in range(5):
        along_z = comp_at(2, comp)
        along_y = comp_at(1, comp)
        total[comp] = (
            flux_z[along_z, pl.ds(16, 128), :] - flux_z[along_z, pl.ds(15, 128), :]
        ).T
        for part in range(16):
            rows = pl.ds(16 + 8 * part, 8)
            flux_x[0, rows, :] = (
                flux_y[along_y, rows, :] - flux_y[along_y, pl.ds(12 + 8 * part, 8), :]
            )
        for x in range(4):
            for part in range(4):
                rows = pl.ds(32 * x + 8 * part, 8)
                total[comp, rows, :] = (
                    total[comp, rows, :]
                    + flux_x[0, pl.ds(16 + 32 * part + x, 8, stride=4), :]
                )

    head_x.wait_recv()
    cells(raw_x, cell_x, 0, 224, 12)
    faces(cell_x, flux_x, 32, 160, 8)
    for copy, plane in zip(tail_x, (2, 1, 0)):
        copy.wait_recv()
        cells(raw_x, cell_x, 0, 32 * plane, 4)
        faces(cell_x, flux_x, 32, 64 + 32 * plane, 4)
    for comp in range(5):
        for part in range(16):
            rows = pl.ds(8 * part, 8)
            total[comp, rows, :] = total[comp, rows, :] + (
                flux_x[comp, pl.ds(96 + 8 * part, 8), :]
                - flux_x[comp, pl.ds(64 + 8 * part, 8), :]
            )

    @pl.when(first_place)
    def _():
        top = tops[1]
        for copy in plane_copies():
            copy.wait_recv()
        for k in range(len(STEPS)):
            top = jnp.maximum(top, top_in[PLANE + k])
        tops[2] = top
        for copy in final_copies():
            copy.start()

    @pl.when(other_place)
    def _():
        top_copy(2, FINAL, 0, device(core, 0, across, gz)).wait_recv()
        tops[2] = top_in[FINAL]

    top = tops[2]
    step = (cfl_number / 12.0) / jnp.max(top, axis=1, keepdims=True)
    for comp in range(5):
        for part in range(16):
            rows = pl.ds(8 * part, 8)
            out_ref[comp, rows, :] = (
                cell_x[comp, pl.ds(96 + 8 * part, 8), :] - step * total[comp, rows, :]
            )
    for copy in halo_z + halo_y + tail_x + [head_x]:
        copy.wait_send()

    @pl.when(other_place)
    def _():
        for flip in range(2):
            first_copy(flip).wait_send()

    @pl.when(first_place)
    def _():
        first_copy(1).wait_send()
        for copy in plane_copies() + final_copies():
            copy.wait_send()


def comp_at(direction, comp):
    if comp in (0, 4):
        return comp
    return 1 + ORDER[direction].index(comp - 1)


def local(density, velocity, pressure):
    f32 = jnp.float32
    result = pl.pallas_call(
        kernel,
        name="section",
        out_shape=pltpu.VMEM((5, 128, 128), f32),
        in_specs=[pl.BlockSpec(memory_space=pltpu.HBM)] * 3,
        out_specs=pl.BlockSpec(memory_space=pltpu.VMEM),
        scratch_shapes=[
            pltpu.VMEM((5, 320, 128), f32),
            pltpu.VMEM((5, 160, 128), f32),
            pltpu.VMEM((5, 160, 128), f32),
            pltpu.VMEM((16, 320, 128), f32),
            pltpu.VMEM((16, 160, 128), f32),
            pltpu.VMEM((16, 160, 128), f32),
            pltpu.VMEM((5, 224, 128), f32),
            pltpu.VMEM((5, 144, 128), f32),
            pltpu.VMEM((5, 144, 128), f32),
            pltpu.VMEM((5, 128, 128), f32),
            pltpu.VMEM((3, 1, 128), f32),
            pltpu.VMEM((FINAL + 1, 1, 128), f32),
            pltpu.SemaphoreType.DMA((5,)),
            pltpu.SemaphoreType.DMA((FINAL + 1,)),
            pltpu.SemaphoreType.DMA((FINAL + 1,)),
            pltpu.SemaphoreType.DMA((8,)),
            pltpu.SemaphoreType.DMA((8,)),
        ],
        compiler_params=pltpu.CompilerParams(collective_id=0, has_side_effects=True),
    )(
        density.reshape(128, 128),
        velocity.reshape(3, 128, 128),
        pressure.reshape(128, 128),
    )
    return result.reshape(5, 4, 32, 128)


def solution(mesh):
    return jax.shard_map(
        local,
        mesh=mesh,
        in_specs=(P("gx", "gy", "gz"), P(None, "gx", "gy", "gz"), P("gx", "gy", "gz")),
        out_specs=P(None, "gx", "gy", "gz"),
        check_vma=False,
    )
```
